256 devices in a mesh: row: 8 (over z_lo, x), col: 32 (over z_hi, y, core).
Axes of the slice: x: 4, y: 4, z: 8 (z_hi: 4, z_lo: 2; z = z_hi * 2 + z_lo), core: 2. Of those that a mesh axis runs over, the one named last changes fastest.
Arguments:
- tokens: bfloat16 [256, 256, 1024], P('row', 'col'), may hold values from -6 to 6
- shifts: int32 [2], replicated, may hold values from 0 to 15
- qkv_weight: bfloat16 [1024, 3, 1024], P('col', None, 'row'), may hold values from -0.1875 to 0.1875
- out_weight: bfloat16 [1024, 1024], P('row', 'col'), may hold values from -0.1875 to 0.1875
- up_weight: bfloat16 [1024, 4096], P('col', 'row'), may hold values from -0.1875 to 0.1875
- down_weight: bfloat16 [4096, 1024], P('row', 'col'), may hold values from -0.09375 to 0.09375
- qk_gain: float32 [1024], P('row'), may hold values from 0.5 to 1.5
- attn_rate: float32 [1024], replicated, may hold values from 0.1 to 0.6
- mlp_rate: float32 [1024], replicated, may hold values from 0.1 to 0.6
- hidden_gain: float32 [4096], P('row'), may hold values from 0.5 to 2
Outputs:
- sphere_out: bfloat16 [256, 256, 1024], P('row', 'col')
The draws below stay inside these ranges and needn't reach their ends.
Inputs may be any that keep to these rules, and one draw needn't show every extreme that they name: shifts[0] offsets the windows along rows, shifts[1] along columns.
All inputs are finite; a program needn't handle non-finite values.
Results may differ from the reference program's by a relative error of at most 0.012.
Values may be sent and summed in bfloat16 or wider, within the bound.
No kernel may reach another device: no remote copies, remote signals or barrier semaphores. Data moves between devices by JAX's collectives and lax.ppermute only.
A program may use at most 128 MiB of HBM per device.

```python
import math
import jax
import jax.numpy as jnp
from jax import lax

D = 1024
H = 16
FF = 4096
HD = 64
WIN = 16
GRID_ROWS = 256
GRID_COLS = 256
N_ROW = 8


def levels(own_key, shape, shards, low, largest):
    def one(axis_at, parts):
        heights = jax.random.uniform(jax.random.fold_in(jax.random.fold_in(own_key, 6), axis_at), (parts,), jnp.float32, low / len(shards), largest / len(shards))
        return jnp.repeat(jnp.exp(heights), shape[axis_at] // parts).reshape((-1,) + (1,) * (len(shape) - axis_at - 1))

    loudness = one(*shards[0])
    for cut in shards[1:]:
        loudness = loudness * one(*cut)
    return loudness


def bell_draw(own_key, dims, scale, limit, shards=(), kind=jnp.bfloat16):
    drawn = scale * jax.random.normal(own_key, dims, jnp.float32)
    if shards:
        drawn = drawn * levels(own_key, dims, shards, -0.22, 0.18)
    return jnp.clip(drawn, -limit, limit).astype(kind)


def setup_inputs(seed: int = 0) -> dict:
    streams_of = jax.random.split(jax.random.key(seed), 11)
    return {
        "tokens": bell_draw(streams_of[0], (GRID_ROWS, GRID_COLS, D), 1.0, 6.0, ((0, 8), (1, 32))),
        "shifts": jax.random.randint(streams_of[1], (2,), 0, WIN).astype(jnp.int32),
        "qkv_weight": bell_draw(streams_of[2], (D, 3, D), D ** -0.5, 0.1875, ((0, 32), (2, 8))),
        "out_weight": bell_draw(streams_of[3], (D, D), D ** -0.5, 0.1875, ((0, 8), (1, 32))),
        "up_weight": bell_draw(streams_of[4], (D, FF), D ** -0.5, 0.1875, ((0, 32), (1, 8))),
        "down_weight": bell_draw(streams_of[5], (FF, D), FF ** -0.5, 0.09375, ((0, 8), (1, 32))),
        "qk_gain": jnp.clip(jnp.exp(math.log(1.5) - 1.0986123 * jax.random.uniform(streams_of[6], (D,), jnp.float32) ** levels(streams_of[6], (D,), ((0, 8),), -0.2, 0.2)), 0.5, 1.5),
        "attn_rate": jnp.clip(jnp.exp(jax.random.uniform(streams_of[7], (D,), jnp.float32, math.log(0.1), math.log(0.6))), 0.1, 0.6),
        "mlp_rate": jnp.clip(jnp.exp(jax.random.uniform(streams_of[8], (D,), jnp.float32, math.log(0.1), math.log(0.6))), 0.1, 0.6),
        "hidden_gain": jnp.clip(jnp.exp(math.log(2.0) - 1.3862944 * jax.random.uniform(streams_of[9], (FF,), jnp.float32) ** levels(streams_of[9], (FF,), ((0, 8),), -0.2, 0.2)), 0.5, 2.0),
    }


def to_sphere(vector):
    return vector * lax.rsqrt(lax.optimization_barrier(jnp.mean(vector * vector, axis=-1, keepdims=True)) + 1e-06)

def rounded(vector):
    return lax.optimization_barrier(vector.astype(jnp.bfloat16)).astype(jnp.float32)

def window_band(operands):
    query_band, key_band, value_band = operands
    scores = jnp.einsum('wqhd,wkhd->whqk', query_band.astype(jnp.float32), key_band.astype(jnp.float32)) / math.sqrt(HD)
    expo = jnp.exp(scores)
    weights = (expo / lax.optimization_barrier(jnp.sum(expo, axis=-1, keepdims=True))).astype(jnp.bfloat16)
    return jnp.einsum('whqk,wkhd->wqhd', weights.astype(jnp.float32), value_band.astype(jnp.float32)).astype(jnp.bfloat16)

def reference(tokens, shifts, qkv_weight, out_weight, up_weight, down_weight, qk_gain, attn_rate, mlp_rate, hidden_gain):
    grid_rows = tokens.shape[0]
    grid_cols = tokens.shape[1]
    token_count = grid_rows * grid_cols
    sphere = to_sphere(tokens.astype(jnp.float32)).reshape(token_count, D)
    sphere_bf = sphere.astype(jnp.bfloat16)
    projected = jnp.dot(sphere_bf, qkv_weight.reshape(D, 3 * D), preferred_element_type=jnp.float32)
    projected = projected.reshape(grid_rows, grid_cols, 3, H, HD)
    head_gain = qk_gain.reshape(H, HD)
    queries = (to_sphere(projected[:, :, 0]) * head_gain).astype(jnp.bfloat16)
    keys_sphere = (to_sphere(projected[:, :, 1]) * head_gain).astype(jnp.bfloat16)
    values = projected[:, :, 2].astype(jnp.bfloat16)
    shift_row = shifts[0]
    shift_col = shifts[1]

    def to_windows(field):
        rolled = jnp.roll(jnp.roll(field, -shift_row, axis=0), -shift_col, axis=1)
        rolled = rolled.reshape(grid_rows // WIN, WIN, grid_cols // WIN, WIN, H, HD)
        return rolled.transpose(0, 2, 1, 3, 4, 5).reshape(grid_rows // WIN, grid_cols // WIN, WIN * WIN, H, HD)
    attended = lax.map(window_band, (to_windows(queries), to_windows(keys_sphere), to_windows(values)))
    attended = attended.reshape(grid_rows // WIN, grid_cols // WIN, WIN, WIN, H, HD)
    attended = attended.transpose(0, 2, 1, 3, 4, 5).reshape(grid_rows, grid_cols, D)
    attended = jnp.roll(jnp.roll(attended, shift_row, axis=0), shift_col, axis=1).reshape(token_count, D)
    group_width = D // N_ROW
    attn_total = jnp.zeros((token_count, D), jnp.float32)
    for group_index in range(N_ROW):
        first = group_index * group_width
        attn_total = attn_total + rounded(jnp.dot(attended[:, first:first + group_width], out_weight[first:first + group_width], preferred_element_type=jnp.float32))
    mixed = to_sphere(sphere + attn_rate * (to_sphere(attn_total) - sphere))
    mixed_bf = mixed.astype(jnp.bfloat16)
    hidden_width = FF // N_ROW
    mlp_total = jnp.zeros((token_count, D), jnp.float32)
    for group_index in range(N_ROW):
        first = group_index * hidden_width
        raised = jnp.dot(mixed_bf, up_weight[:, first:first + hidden_width], preferred_element_type=jnp.float32) * hidden_gain[first:first + hidden_width]
        activated = jax.nn.gelu(raised, approximate=False).astype(jnp.bfloat16)
        mlp_total = mlp_total + rounded(jnp.dot(activated, down_weight[first:first + hidden_width], preferred_element_type=jnp.float32))
    sphere_out = to_sphere(mixed + mlp_rate * (to_sphere(mlp_total) - mixed))
    return sphere_out.astype(jnp.bfloat16).reshape(grid_rows, grid_cols, D)
```

```python
import math

import jax
import jax.numpy as jnp
from jax import lax
from jax.sharding import Mesh, PartitionSpec as P

HD = 64
WIN = 16
ROW = ("zlo", "x")
COL = ("zhi", "y", "core")
Z = ("zlo", "zhi")


def to_sphere(vector):
    return vector * lax.rsqrt(jnp.mean(vector * vector, axis=-1, keepdims=True) + 1e-06)


def from_offset(value, axis, offset):
    n = lax.axis_size(axis)
    return lax.ppermute(value, axis, [((i + offset) % n, i) for i in range(n)])


def swapped(value):
    return lax.ppermute(value, "core", [(0, 1), (1, 0)])


def from_z(value, dzlo, dzhi):
    pairs = [
        ((zl ^ dzlo) * 4 + (zh + dzhi) % 4, zl * 4 + zh) for zl in range(2) for zh in range(4)
    ]
    return lax.ppermute(value, Z, pairs)


def ring_z(value, step):
    def flat(z):
        return (z % 2) * 4 + z // 2

    return lax.ppermute(value, Z, [(flat((z + step) % 8), flat(z)) for z in range(8)])


def gather_z(value):
    blocks = [
        value if (a, b) == (0, 0) else from_z(value, a, b) for a in range(2) for b in range(4)
    ]
    return jnp.stack(blocks).reshape(2, 4, *value.shape)


def direct4(value, axis):
    return jnp.stack([value] + [from_offset(value, axis, d) for d in (1, 2, 3)])


def ring4(value, axis):
    half = value.shape[0] // 2
    nxt = from_offset(value, axis, 1)
    prv = from_offset(value, axis, -1)
    far_a = from_offset(prv[:half], axis, -1)
    far_b = from_offset(nxt[half:], axis, 1)
    return jnp.stack([value, nxt, jnp.concatenate([far_a, far_b]), prv])


def ring8_z(value):
    up, down = [value], [value]
    for _ in range(3):
        up.append(ring_z(up[-1], 1))
        down.append(ring_z(down[-1], -1))
    half = value.shape[0] // 2
    far = jnp.concatenate([ring_z(down[-1][:half], -1), ring_z(up[-1][half:], 1)])
    return up[:4] + [far] + [down[3], down[2], down[1]]


def on_device(
    tokens, shifts, qkv_weight, out_weight, up_weight, down_weight, qk_gain, attn_rate, mlp_rate, hidden_gain
):
    core = lax.axis_index("core")
    zlo = lax.axis_index("zlo")
    zhi = lax.axis_index("zhi")
    y = lax.axis_index("y")
    rows, cols, width = tokens.shape
    first = core == 0

    out_t = out_weight.T
    down_t = down_weight.T

    def half(h):
        lo, hi = h * 64, h * 64 + 64
        return jnp.concatenate(
            [
                qkv_weight[:, 0, lo:hi],
                qkv_weight[:, 1, lo:hi],
                qkv_weight[:, 2, lo:hi],
                out_t[:, lo:hi],
                up_weight[:, 256 * h : 256 * h + 256],
                down_t[:, 256 * h : 256 * h + 256],
            ],
            axis=-1,
        )

    half0, half1 = half(0), half(1)
    keep = jnp.where(first, half0, half1)
    other = swapped(jnp.where(first, half1, half0))
    shard = jnp.concatenate([jnp.where(first, keep, other), jnp.where(first, other, keep)], 0)

    zc = gather_z(shard[:, :256])
    zd = gather_z(shard[:, 512:])
    qk = ring4(direct4(zc[..., :128], "y"), "x")
    vo = ring4(direct4(zc[..., 128:], "x"), "y")
    d1 = ring4(direct4(zd[..., :128], "y"), "x")
    d2 = ring4(direct4(zd[..., 128:], "x"), "y")
    up_blocks = ring8_z(direct4(direct4(shard[:, 256:512], "x"), "y"))
    up_even = jnp.stack(up_blocks[0::2])
    up_odd = jnp.stack(up_blocks[1::2])
    up_odd = jnp.where(zlo == 0, up_odd, jnp.roll(up_odd, 1, axis=0))

    gains = jnp.concatenate([qk_gain, hidden_gain])
    gains = jnp.stack([gains, lax.ppermute(gains, "zlo", [(0, 1), (1, 0)])])
    gains = jnp.moveaxis(direct4(gains, "x"), 0, 1)
    head_gain = lax.dynamic_slice_in_dim(gains, core * 64, 64, 2).reshape(8, 64)
    unit_gain = lax.dynamic_slice_in_dim(gains, 128 + core * 256, 256, 2).reshape(2048)

    nxt_rows = from_offset(tokens[:WIN], ROW, 1)
    rolled = lax.dynamic_slice_in_dim(jnp.concatenate([tokens, nxt_rows], 0), shifts[0], rows, 0)
    nxt_cols = from_offset(rolled, COL, 2)
    mine = jnp.stack([rolled, nxt_cols])
    theirs = swapped(mine)
    left, right = jnp.where(first, mine, theirs), jnp.where(first, theirs, mine)
    ext = jnp.concatenate([left[0], right[0], left[1], right[1]], axis=1)
    win = lax.dynamic_slice_in_dim(ext, shifts[1], WIN, 1).reshape(2 * WIN * WIN, width)

    def relative(v):
        v = v.reshape(*v.shape[:-1], 4, 4, 64)
        return jnp.roll(jnp.roll(v, -zhi, axis=-3), -y, axis=-2).reshape(*v.shape[:-3], width)

    def absolute(v):
        v = v.reshape(*v.shape[:-1], 4, 4, 64)
        return jnp.roll(jnp.roll(v, zhi, axis=-3), y, axis=-2).reshape(*v.shape[:-3], width)

    xw = to_sphere(relative(win).astype(jnp.float32)).astype(jnp.bfloat16).reshape(512, 4, 4, 64)
    f32 = dict(preferred_element_type=jnp.float32)
    pqk = jnp.einsum("tzyi,xyazin->taxn", xw, qk, **f32).reshape(2, 256, 8, 2, 64)
    pv = jnp.einsum("tzyi,yxazin->taxn", xw, vo[..., :64], **f32).reshape(2, 256, 8, 64)
    q = (to_sphere(pqk[:, :, :, 0]) * head_gain).astype(jnp.bfloat16)
    k = (to_sphere(pqk[:, :, :, 1]) * head_gain).astype(jnp.bfloat16)
    v = pv.astype(jnp.bfloat16)
    score = jnp.einsum("wqhd,wkhd->whqk", q, k, **f32) / math.sqrt(HD)
    expo = jnp.exp(score)
    weights = (expo / jnp.sum(expo, axis=-1, keepdims=True)).astype(jnp.bfloat16)
    att = jnp.einsum("whqk,wkhd->wqhd", weights, v, **f32).astype(jnp.bfloat16)
    att = att.reshape(512, 2, 4, 64)
    part = jnp.einsum("taxn,yxazin->tzyi", att, vo[..., 64:], **f32).reshape(2, 256, width)

    def summed(part):
        own = jnp.where(first, part[0], part[1])
        sent = jnp.where(first, part[1], part[0]).astype(jnp.bfloat16)
        return own + swapped(sent).astype(jnp.float32)

    attn_win = absolute(summed(part).astype(jnp.bfloat16)).reshape(WIN, WIN, width)
    prev_cols = from_offset(attn_win, COL, -2)
    both = jnp.concatenate([prev_cols, attn_win], 1)
    tile = lax.dynamic_slice_in_dim(both, WIN - shifts[1], WIN, 1)
    own_cols = jnp.where(first, tile[:, :8], tile[:, 8:])
    sent_cols = swapped(jnp.where(first, tile[:, 8:], tile[:, :8]))
    strip = jnp.concatenate(
        [jnp.where(first, own_cols, sent_cols), jnp.where(first, sent_cols, own_cols)], 0
    )
    prev_rows = from_offset(strip[WIN:], ROW, -1)
    attn = lax.dynamic_slice_in_dim(jnp.concatenate([prev_rows, strip], 0), WIN - shifts[0], rows, 0)
    attn = relative(attn.reshape(256, width)).astype(jnp.float32)

    sphere = to_sphere(relative(tokens.reshape(256, width)).astype(jnp.float32))
    rate_a, rate_m = relative(attn_rate), relative(mlp_rate)
    mixed = to_sphere(sphere + rate_a * (to_sphere(attn) - sphere))
    mine = mixed.astype(jnp.bfloat16)
    theirs = swapped(mine)
    mx = jnp.stack([jnp.where(first, mine, theirs), jnp.where(first, theirs, mine)])
    mx = mx.reshape(512, 4, 4, 64)
    raised = jnp.stack(
        [jnp.einsum("tzyi,zyxin->txn", mx, w, **f32) for w in (up_even, up_odd)], 1
    ).reshape(512, 2048)
    act = jax.nn.gelu(raised * unit_gain, approximate=False).astype(jnp.bfloat16)
    act = act.reshape(512, 2, 4, 256)
    part = jnp.einsum("taxk,xyazik->tzyi", act[..., :128], d1, **f32) + jnp.einsum(
        "taxk,yxazik->tzyi", act[..., 128:], d2, **f32
    )
    mlp = summed(part.reshape(2, 256, width))
    res = to_sphere(mixed + rate_m * (to_sphere(mlp) - mixed)).astype(jnp.bfloat16)
    return absolute(res).reshape(rows, cols, width)


def solution(mesh):
    fine = Mesh(mesh.devices.reshape(2, 4, 4, 4, 2), ("zlo", "x", "zhi", "y", "core"))
    return jax.shard_map(
        on_device,
        mesh=fine,
        in_specs=(
            P(ROW, COL, None),
            P(),
            P(COL, None, ROW),
            P(ROW, COL),
            P(COL, ROW),
            P(ROW, COL),
            P(ROW),
            P(),
            P(),
            P(ROW),
        ),
        out_specs=P(ROW, COL, None),
        check_vma=False,
    )
```

```python
import jax
import jax.numpy as jnp
from jax import lax
from jax.experimental import pallas as pl
from jax.experimental.pallas import tpu as pltpu
from jax.sharding import Mesh, PartitionSpec as P


HD = 64
WIN = 16
ROW = ("zlo", "x")
COL = ("zhi", "y", "core")
Z = ("zlo", "zhi")
F32 = jnp.float32
BF16 = jnp.bfloat16
NT = (((1,), (1,)), ((), ()))


def from_offset(value, axis, offset):
    n = lax.axis_size(axis)
    return lax.ppermute(value, axis, [((i + offset) % n, i) for i in range(n)])


def swapped(value, axis="core"):
    return lax.ppermute(value, axis, [(0, 1), (1, 0)])


def ring_z(value, step):
    def flat(z):
        return (z % 2) * 4 + z // 2

    return lax.ppermute(value, Z, [(flat((z + step) % 8), flat(z)) for z in range(8)])


def across_edge(value):
    n = lax.axis_size(COL)
    pairs = [((c - 1 if c % 2 == 0 else c + 1) % n, c) for c in range(n)]
    return lax.ppermute(value, COL, pairs)


def direct4(value, axis):
    return [value] + [from_offset(value, axis, d) for d in (1, 2, 3)]


def ring8_z(value):
    up, down = [value], [value]
    for _ in range(4):
        up.append(ring_z(up[-1], 1))
    for _ in range(3):
        down.append(ring_z(down[-1], -1))
    return up + [down[3], down[2], down[1]]


def call(kernel, outs, *args, scratch=(), space=pltpu.VMEM):
    specs = [pl.BlockSpec(memory_space=pltpu.SMEM)] + [
        pl.BlockSpec(memory_space=space) for _ in args[1:]
    ]
    single = not isinstance(outs, (list, tuple))
    out = pl.pallas_call(
        kernel,
        out_shape=outs,
        in_specs=specs,
        out_specs=jax.tree.map(lambda _: pl.BlockSpec(memory_space=pltpu.VMEM), outs),
        scratch_shapes=list(scratch),
        compiler_params=pltpu.CompilerParams(vmem_limit_bytes=48 * 2**20),
    )(*args)
    return out if single else tuple(out)


def sds(shape, dtype):
    return jax.ShapeDtypeStruct(shape, dtype)


def norm(v):
    return v * lax.rsqrt(jnp.mean(v * v, axis=-1, keepdims=True) + 1e-06)


def to_relative(v, y):
    return pltpu.roll(v, lax.rem(256 - 64 * y, 256), 1)


def to_absolute(v, y):
    return pltpu.roll(v, 64 * y, 1)


def pack_kernel(pos, *refs):
    sources, (keep, send, gains), local, arrived = refs[:6], refs[6:9], refs[9:15], refs[15]
    copies = [
        pltpu.make_async_copy(a, b, arrived.at[i]) for i, (a, b) in enumerate(zip(sources, local))
    ]
    for copy in copies:
        copy.start()
    for copy in copies:
        copy.wait()
    qkv, out_t, up, down_t, qk_gain, hidden_gain = local
    first = pos[0] == 0

    def put(i, lo, hi):
        keep[i] = jnp.where(first, lo, hi)
        send[i] = jnp.where(first, hi, lo)

    q, k, v, o = qkv[0].astype(F32), qkv[1].astype(F32), qkv[2].astype(F32), out_t[...].astype(F32)

    def pair(i, a, b):
        lo = jnp.concatenate([a[:, :64], b[:, :64]], 1).astype(BF16)
        hi = jnp.concatenate([a[:, 64:], b[:, 64:]], 1).astype(BF16)
        put(i, lo, hi)

    pair(0, q, k)
    put(1, down_t[:, :128], down_t[:, 256:384])
    pair(2, v, o)
    put(3, down_t[:, 128:256], down_t[:, 384:])
    put(4, up[:, :128], up[:, 256:384])
    put(5, up[:, 128:256], up[:, 384:])
    g = qk_gain[...]
    lane = lax.broadcasted_iota(jnp.int32, g.shape, 1)
    turned = pltpu.roll(g, HD, 1)
    g = jnp.where(first == (lane < HD), g, turned)
    h = hidden_gain[...]
    rest = jnp.concatenate([g, jnp.where(first, h[:2], h[2:]), jnp.zeros((5, 128), F32)], 0)
    for i in range(3):
        part = rest.astype(BF16)
        rest = rest - part.astype(F32)
        gains[8 * i : 8 * i + 8] = part.astype(F32)
    gains[24:] = jnp.zeros((8, 128), F32)


def rows_kernel(pos, keep, recv, gains, wide, up):
    mine = pl.multiple_of(pos[0] * 32, 32)
    other = pl.multiple_of(32 - pos[0] * 32, 32)
    for i in range(6):
        out, base = (wide, 64 * i) if i < 4 else (up, 64 * (i - 4))
        out[pl.ds(base + mine, 32)] = keep[i]
        out[pl.ds(base + other, 32)] = recv[i]
    wide[256:] = gains[...].astype(BF16)


def attn_kernel(pos, win, gain, *refs):
    qk, vo, part, xs = refs[:4], refs[4:8], refs[8], refs[9]
    zhi, y = pos[2], pos[3]
    s = norm(win[...].astype(F32))
    for z in range(4):
        slab = to_relative(s[:, 256 * z : 256 * z + 256], y)
        xs[lax.rem(z + 4 - zhi, 4)] = slab.astype(BF16)
    x = jnp.concatenate([xs[i] for i in range(4)], 1)
    group = lax.broadcasted_iota(jnp.int32, (256, 256), 0) // HD
    mean = jnp.where(group == lax.broadcasted_iota(jnp.int32, (256, 256), 1) // HD, 1 / HD, 0.0)
    mean = mean.astype(BF16)
    lane = lax.broadcasted_iota(jnp.int32, (512, 128), 1)
    ones = jnp.ones((256, 128), BF16)
    zero = jnp.zeros((512, 128), F32)
    head_out = [[None] * 8, [None] * 8]
    for dx in range(4):

        def stacked(block):
            return jnp.concatenate(
                [
                    jnp.concatenate([block(z, dy, a) for z in range(4) for dy in range(4)], 0)
                    for a in range(2)
                ],
                1,
            )

        wqk = stacked(lambda z, dy, a: qk[dx][dy, z, a])
        wvo = stacked(lambda z, dy, a: vo[dy][dx, z, a])
        pqk = jnp.dot(x, wqk, preferred_element_type=F32)
        pv = jnp.dot(x, wvo, preferred_element_type=F32)
        square = pqk * pqk
        high = square.astype(BF16)
        low = (square - high.astype(F32)).astype(BF16)
        level = jnp.dot(high, mean, preferred_element_type=F32)
        level = level + jnp.dot(low, mean, preferred_element_type=F32)
        pqk = pqk * lax.rsqrt(level + 1e-06)
        for a in range(2):
            both = pqk[:, 128 * a : 128 * a + 128] * gain[a * 4 + dx][None]
            query = jnp.where(lane < HD, both * (HD**-0.5), zero).astype(BF16)
            key = pltpu.roll(both, HD, 1).astype(BF16)
            v = pltpu.roll(pv[:, 128 * a : 128 * a + 128], HD, 1)
            v = jnp.where(lane < HD, zero, v).astype(BF16)
            for w in range(2):
                t = slice(256 * w, 256 * w + 256)
                e = jnp.exp(lax.dot_general(query[t], key[t], NT, preferred_element_type=F32))
                o = jnp.dot(
                    e.astype(BF16), jnp.concatenate([v[t], ones], 1), preferred_element_type=F32
                )
                head_out[w][a * 4 + dx] = (o[:, :128] / o[:, 128:]).astype(BF16)
    att = jnp.concatenate([jnp.concatenate(h, 1) for h in head_out], 0)
    for z in range(4):
        rhs = jnp.concatenate(
            [
                jnp.concatenate([vo[dy][dx, z, a] for dy in range(4)], 0)
                for a in range(2)
                for dx in range(4)
            ],
            1,
        )
        r = lax.dot_general(att, rhs, NT, preferred_element_type=F32)
        at = pl.multiple_of(lax.rem(z + zhi, 4) * 256, 256)
        part[:, pl.ds(at, 256)] = to_absolute(r, y).astype(BF16)


def mix_kernel(pos, tokens, attn, rate, mixed, mx):
    zhi, y = pos[2], pos[3]
    s = norm(tokens[...].astype(F32))
    m = norm(s + rate[...] * (norm(attn[...].astype(F32)) - s))
    mixed[...] = m
    for z in range(4):
        slab = to_relative(m[:, 256 * z : 256 * z + 256], y)
        mx[lax.rem(z + 4 - zhi, 4)] = slab.astype(BF16)


def up_kernel(pos, own, other, gain, *refs):
    blocks, act = refs[:8], refs[8]
    zlo, y, across = pos[1], pos[3], pos[4]

    def turn(at, d):
        return lax.bitwise_xor(lax.rem(at + d, 4), at)

    for a in range(2):
        slabs = [lax.rem(m + a * zlo, 4) for m in range(4)]
        x = jnp.concatenate(
            [jnp.concatenate([half[i] for i in slabs], 1) for half in (own, other)], 0
        )
        for dx in range(4):
            w = jnp.concatenate(
                [
                    jnp.concatenate(
                        [blocks[2 * m + a][turn(y, dy), turn(across, dx), n] for m in range(4) for dy in range(4)], 0
                    )
                    for n in range(2)
                ],
                1,
            )
            unit = a * 4 + dx
            r = jnp.dot(x, w, preferred_element_type=F32) * gain[unit][None]
            r = 0.5 * r * (1.0 + lax.erf(r * (0.5**0.5)))
            act[:, 256 * unit : 256 * unit + 256] = r.astype(BF16)


def down_kernel(pos, act, *refs):
    lo, hi, own, other = refs[:4], refs[4:8], refs[8], refs[9]
    zhi, y = pos[2], pos[3]
    x = act[...]
    for z in range(4):
        rhs = []
        for a in range(2):
            for dx in range(4):
                rhs.append(jnp.concatenate([lo[dx][dy, z, a] for dy in range(4)], 0))
                rhs.append(jnp.concatenate([hi[dy][dx, z, a] for dy in range(4)], 0))
        r = lax.dot_general(x, jnp.concatenate(rhs, 1), NT, preferred_element_type=F32)
        r = to_absolute(r, y)
        at = pl.multiple_of(lax.rem(z + zhi, 4) * 256, 256)
        own[:, pl.ds(at, 256)] = r[:256]
        other[:, pl.ds(at, 256)] = r[256:].astype(BF16)


def last_kernel(pos, own, recv, mixed, rate, out):
    m = mixed[...]
    mlp = own[...] + recv[...].astype(F32)
    out[...] = norm(m + rate[...] * (norm(mlp) - m)).astype(BF16)


def layer(
    tokens, shifts, qkv_weight, out_weight, up_weight, down_weight, qk_gain, attn_rate, mlp_rate, hidden_gain
):
    core = lax.axis_index("core")
    first = core == 0
    pos = jnp.stack([core] + [lax.axis_index(n) for n in ("zlo", "zhi", "y", "x")])
    pos = pos.astype(jnp.int32)
    rows, cols, width = tokens.shape
    count = rows * cols

    six = sds((6, 32, 128), BF16)
    keep, send, gains = call(
        pack_kernel,
        (six, six, sds((32, 128), F32)),
        pos,
        jnp.transpose(qkv_weight, (1, 0, 2)),
        out_weight.T,
        up_weight,
        down_weight.T,
        qk_gain.reshape(1, 128),
        hidden_gain.reshape(4, 128),
        scratch=[
            pltpu.VMEM((3, 32, 128), BF16),
            pltpu.VMEM((32, 128), BF16),
            pltpu.VMEM((32, 512), BF16),
            pltpu.VMEM((32, 512), BF16),
            pltpu.VMEM((1, 128), F32),
            pltpu.VMEM((4, 128), F32),
            pltpu.SemaphoreType.DMA((6,)),
        ],
        space=pltpu.HBM,
    )
    wide, up = call(
        rows_kernel, (sds((288, 128), BF16), sds((128, 128), BF16)), pos, keep, swapped(send), gains
    )

    pair = jnp.stack([wide, swapped(wide, "zlo")])
    gains = pair[:, 256:]
    quad = direct4(pair[:, :256], "zhi")
    one = jnp.stack([b[:, :128] for b in quad])
    two = jnp.concatenate([b[:, 128:].reshape(256, 128) for b in quad] + [gains.reshape(64, 128)])
    one = direct4(one, "y")
    two = direct4(two, "x")
    gains = jnp.stack([b[1024:].reshape(2, 4, 8, 128) for b in two], 1).astype(F32)
    gains = gains[:, :, 0] + gains[:, :, 1] + gains[:, :, 2]
    head_gain = gains[:, :, 0].reshape(8, 128)
    unit_gain = gains[:, :, 1:3].reshape(8, 256)
    two = [b[:1024].reshape(4, 2, 128, 128) for b in two]
    qk = direct4(jnp.stack([b[:, :, :64] for b in one]), "x")
    vo = direct4(jnp.stack([b[:, :, :64] for b in two]), "y")
    d_lo = direct4(jnp.stack([b[:, :, 64:] for b in one]), "x")
    d_hi = direct4(jnp.stack([b[:, :, 64:] for b in two]), "y")
    for axis in ("x", "y"):
        for step in (1, 2):
            pairs = [(i ^ step, i) for i in range(4)]
            up = jnp.stack([up, lax.ppermute(up, axis, pairs)])
    up_z = ring8_z(up.reshape(4, 4, 2, 64, 128))

    shift_row = shifts[0]
    shift_col = jnp.where(shifts[1] > 8, shifts[1] - WIN, shifts[1])
    nxt_rows = from_offset(tokens[:WIN], ROW, 1)
    rolled = lax.dynamic_slice_in_dim(jnp.concatenate([tokens, nxt_rows], 0), shift_row, rows, 0)
    mine = jnp.stack([rolled, across_edge(rolled)])
    theirs = swapped(mine)
    left, right = jnp.where(first, mine, theirs), jnp.where(first, theirs, mine)
    ext = jnp.concatenate([left[1], left[0], right[0], right[1]], axis=1)
    win = lax.dynamic_slice_in_dim(ext, cols + shift_col, WIN, 1).reshape(2 * count, width)

    part = call(
        attn_kernel,
        sds((2 * count, width), BF16),
        pos,
        win,
        head_gain,
        *qk,
        *vo,
        scratch=[pltpu.VMEM((4, 2 * count, 256), BF16)],
    )
    full = (part.astype(F32) + swapped(part).astype(F32)).astype(BF16)
    full = full.reshape(rows, WIN, width)

    halo = across_edge(jnp.where(first, full[:, :cols], full[:, cols:]))
    ext = jnp.where(
        first, jnp.concatenate([halo, full], axis=1), jnp.concatenate([full, halo], axis=1)
    )
    strip = lax.dynamic_slice_in_dim(ext, cols - shift_col, cols, 1)
    prev_rows = from_offset(strip[rows - WIN :], ROW, -1)
    attn = lax.dynamic_slice_in_dim(
        jnp.concatenate([prev_rows, strip], 0), WIN - shift_row, rows, 0
    ).reshape(count, width)

    mixed, mx = call(
        mix_kernel,
        (sds((count, width), F32), sds((4, count, 256), BF16)),
        pos,
        tokens.reshape(count, width),
        attn,
        attn_rate.reshape(1, width),
    )
    act = call(up_kernel, sds((2 * count, 2048), BF16), pos, mx, swapped(mx), unit_gain, *up_z)
    own, other = call(
        down_kernel, (sds((count, width), F32), sds((count, width), BF16)), pos, act, *d_lo, *d_hi
    )
    result = call(
        last_kernel,
        sds((count, width), BF16),
        pos,
        own,
        swapped(other),
        mixed,
        mlp_rate.reshape(1, width),
    )
    return result.reshape(rows, cols, width)


def solution(mesh):
    fine = Mesh(mesh.devices.reshape(2, 4, 4, 4, 2), ("zlo", "x", "zhi", "y", "core"))
    return jax.shard_map(
        layer,
        mesh=fine,
        in_specs=(
            P(ROW, COL, None),
            P(),
            P(COL, None, ROW),
            P(ROW, COL),
            P(COL, ROW),
            P(ROW, COL),
            P(ROW),
            P(),
            P(),
            P(ROW),
        ),
        out_specs=P(ROW, COL, None),
        check_vma=False,
    )
```

```python
import jax
import jax.numpy as jnp
from jax import lax
from jax.experimental import pallas as pl
from jax.experimental.pallas import tpu as pltpu
from jax.sharding import Mesh, PartitionSpec as P


HD = 64
WIN = 16
ROW = ("zlo", "x")
COL = ("zhi", "y", "core")
F32 = jnp.float32
BF16 = jnp.bfloat16
NT = (((1,), (1,)), ((), ()))


def from_offset(value, axis, offset):
    n = lax.axis_size(axis)
    return lax.ppermute(value, axis, [((i + offset) % n, i) for i in range(n)])


def swapped(value, axis="core"):
    return lax.ppermute(value, axis, [(0, 1), (1, 0)])


def across_edge(value):
    n = lax.axis_size(COL)
    pairs = [((c - 1 if c % 2 == 0 else c + 1) % n, c) for c in range(n)]
    return lax.ppermute(value, COL, pairs)


def direct4(value, axis):
    return [value] + [from_offset(value, axis, d) for d in (1, 2, 3)]


def ring4(value, axis):
    nxt = from_offset(value, axis, 1)
    prv = from_offset(value, axis, -1)
    return [value, nxt, from_offset(nxt, axis, 1), prv]


def call(kernel, outs, *args, scratch=()):
    specs = [pl.BlockSpec(memory_space=pltpu.SMEM)] + [
        pl.BlockSpec(memory_space=pltpu.VMEM) for _ in args[1:]
    ]
    single = not isinstance(outs, (list, tuple))
    out = pl.pallas_call(
        kernel,
        out_shape=outs,
        in_specs=specs,
        out_specs=jax.tree.map(lambda _: pl.BlockSpec(memory_space=pltpu.VMEM), outs),
        scratch_shapes=list(scratch),
        compiler_params=pltpu.CompilerParams(vmem_limit_bytes=48 * 2**20),
    )(*args)
    return out if single else tuple(out)


def sds(shape, dtype):
    return jax.ShapeDtypeStruct(shape, dtype)


def norm(v):
    return v * lax.rsqrt(jnp.mean(v * v, axis=-1, keepdims=True) + 1e-06)


def to_relative(v, y):
    return pltpu.roll(v, lax.rem(256 - 64 * y, 256), 1)


def to_absolute(v, y):
    return pltpu.roll(v, 64 * y, 1)


def pack_kernel(pos, qkv, out_t, up, down_t, keep, send):
    first = pos[0] == 0

    def put(i, lo, hi):
        keep[i] = jnp.where(first, lo, hi)
        send[i] = jnp.where(first, hi, lo)

    q, k, v, o = qkv[0].astype(F32), qkv[1].astype(F32), qkv[2].astype(F32), out_t[...].astype(F32)

    def pair(i, a, b):
        lo = jnp.concatenate([a[:, :64], b[:, :64]], 1).astype(BF16)
        hi = jnp.concatenate([a[:, 64:], b[:, 64:]], 1).astype(BF16)
        put(i, lo, hi)

    pair(0, q, k)
    put(1, down_t[:, :128], down_t[:, 256:384])
    put(2, up[:, :128], up[:, 256:384])
    pair(3, v, o)
    put(4, down_t[:, 128:256], down_t[:, 384:])
    put(5, up[:, 128:256], up[:, 384:])


def rows_kernel(pos, keep, recv, qk_gain, hidden_gain, wide):
    first = pos[0] == 0
    mine = pl.multiple_of(pos[0] * 32, 32)
    other = pl.multiple_of(32 - pos[0] * 32, 32)
    for i in range(6):
        wide[pl.ds(64 * i + mine, 32)] = keep[i]
        wide[pl.ds(64 * i + other, 32)] = recv[i]
    g = qk_gain[...]
    lane = lax.broadcasted_iota(jnp.int32, g.shape, 1)
    turned = pltpu.roll(g, HD, 1)
    g = jnp.where(first == (lane < HD), g, turned)
    h = hidden_gain[...]
    rest = jnp.concatenate([g, jnp.where(first, h[:2], h[2:]), jnp.zeros((5, 128), F32)], 0)
    parts = []
    for _ in range(3):
        parts.append(rest.astype(BF16).astype(F32))
        rest = rest - parts[-1]
    parts.append(jnp.zeros((8, 128), F32))
    wide[384:] = jnp.concatenate(parts, 0).astype(BF16)


def attn_kernel(pos, win, gain, *refs):
    qk, vo, part, (xs, qs, ks, vs, att) = refs[:4], refs[4:8], refs[8], refs[9:]
    zhi, y = pos[2], pos[3]
    s = norm(win[...].astype(F32))
    for z in range(4):
        slab = to_relative(s[:, 256 * z : 256 * z + 256], y)
        xs[lax.rem(z + 4 - zhi, 4)] = slab.astype(BF16)
    x = jnp.concatenate([xs[i] for i in range(4)], 1)
    group = lax.broadcasted_iota(jnp.int32, (256, 256), 0) // HD
    mean = jnp.where(group == lax.broadcasted_iota(jnp.int32, (256, 256), 1) // HD, 1 / HD, 0.0)
    mean = mean.astype(BF16)
    lane = lax.broadcasted_iota(jnp.int32, (512, 128), 1)
    ones = jnp.ones((256, 128), BF16)
    zero = jnp.zeros((512, 128), F32)
    for dx in range(4):

        def stacked(block):
            return jnp.concatenate(
                [
                    jnp.concatenate([block(z, dy, a) for z in range(4) for dy in range(4)], 0)
                    for a in range(2)
                ],
                1,
            )

        wqk = stacked(lambda z, dy, a: qk[dx][dy, z, a])
        wvo = stacked(lambda z, dy, a: vo[dy][dx, z, a])
        pqk = jnp.dot(x, wqk, preferred_element_type=F32)
        pv = jnp.dot(x, wvo, preferred_element_type=F32)
        square = pqk * pqk
        high = square.astype(BF16)
        low = (square - high.astype(F32)).astype(BF16)
        level = jnp.dot(high, mean, preferred_element_type=F32)
        level = level + jnp.dot(low, mean, preferred_element_type=F32)
        pqk = pqk * lax.rsqrt(level + 1e-06)
        for a in range(2):
            both = pqk[:, 128 * a : 128 * a + 128] * gain[a * 4 + dx][None]
            head = a * 4 + dx
            qs[head] = jnp.where(lane < HD, both * (HD**-0.5), zero).astype(BF16)
            ks[head] = pltpu.roll(both, HD, 1).astype(BF16)
            v = pltpu.roll(pv[:, 128 * a : 128 * a + 128], HD, 1)
            vs[head] = jnp.where(lane < HD, zero, v).astype(BF16)

    def heads(i, carry):
        for head in (2 * i, 2 * i + 1):
            for w in range(2):
                t = slice(256 * w, 256 * w + 256)
                score = lax.dot_general(qs[head, t], ks[head, t], NT, preferred_element_type=F32)
                e = jnp.exp(score).astype(BF16)
                rhs = jnp.concatenate([vs[head, t], ones], 1)
                o = jnp.dot(e, rhs, preferred_element_type=F32)
                at = pl.multiple_of(128 * head, 128)
                att[t, pl.ds(at, 128)] = (o[:, :128] / o[:, 128:]).astype(BF16)
        return carry

    lax.fori_loop(0, 4, heads, 0)

    def project(z, carry):
        rhs = jnp.concatenate(
            [
                jnp.concatenate([vo[dy][dx, z, a] for dy in range(4)], 0)
                for a in range(2)
                for dx in range(4)
            ],
            1,
        )
        r = lax.dot_general(att[...], rhs, NT, preferred_element_type=F32)
        at = pl.multiple_of(lax.rem(z + zhi, 4) * 256, 256)
        part[:, pl.ds(at, 256)] = to_absolute(r, y).astype(BF16)
        return carry

    lax.fori_loop(0, 4, project, 0)


def mix_kernel(pos, tokens, attn, rate, mixed, mx):
    zhi, y = pos[2], pos[3]

    def chunk(i, carry):
        t = pl.ds(pl.multiple_of(128 * i, 128), 128)
        s = norm(tokens[t].astype(F32))
        m = norm(s + rate[...] * (norm(attn[t].astype(F32)) - s))
        mixed[t] = m
        for z in range(4):
            slab = to_relative(m[:, 256 * z : 256 * z + 256], y)
            mx[lax.rem(z + 4 - zhi, 4), t] = slab.astype(BF16)
        return carry

    lax.fori_loop(0, 2, chunk, 0)


def up_kernel(pos, own, other, gain, *refs):
    over_x, over_y, act = refs[:4], refs[4:8], refs[8]
    x = jnp.concatenate(
        [jnp.concatenate([half[z] for z in range(4)], 1) for half in (own, other)], 0
    )
    for a in range(2):
        for dx in range(4):
            blocks = [(z, dy) for z in range(4) for dy in range(4)]
            w = jnp.concatenate(
                [
                    jnp.concatenate(
                        [over_x[dx][1, dy, z, a] for z, dy in blocks], 0
                    ),
                    jnp.concatenate(
                        [over_y[dy][1, dx, z, a] for z, dy in blocks], 0
                    ),
                ],
                1,
            )
            unit = a * 4 + dx
            r = jnp.dot(x, w, preferred_element_type=F32) * gain[unit][None]
            r = 0.5 * r * (1.0 + lax.erf(r * (0.5**0.5)))
            act[:, 256 * unit : 256 * unit + 256] = r.astype(BF16)


def down_kernel(pos, act, *refs):
    over_x, over_y, own, other = refs[:4], refs[4:8], refs[8], refs[9]
    zhi, y = pos[2], pos[3]

    x = act[...]
    for z in range(4):
        rhs = []
        for a in range(2):
            for dx in range(4):
                lo = [over_x[dx][0, dy, z, a] for dy in range(4)]
                hi = [over_y[dy][0, dx, z, a] for dy in range(4)]
                rhs += [jnp.concatenate(lo, 0), jnp.concatenate(hi, 0)]
        r = lax.dot_general(x, jnp.concatenate(rhs, 1), NT, preferred_element_type=F32)
        r = to_absolute(r, y)
        at = pl.multiple_of(lax.rem(z + zhi, 4) * 256, 256)
        own[:, pl.ds(at, 256)] = r[:256]
        other[:, pl.ds(at, 256)] = r[256:].astype(BF16)


def last_kernel(pos, own, recv, mixed, rate, out):
    def chunk(i, carry):
        t = pl.ds(pl.multiple_of(128 * i, 128), 128)
        m = mixed[t]
        mlp = own[t] + recv[t].astype(F32)
        out[t] = norm(m + rate[...] * (norm(mlp) - m)).astype(BF16)
        return carry

    lax.fori_loop(0, 2, chunk, 0)


def layer(
    tokens, shifts, qkv_weight, out_weight, up_weight, down_weight, qk_gain, attn_rate, mlp_rate, hidden_gain
):
    core = lax.axis_index("core")
    first = core == 0
    pos = jnp.stack([core] + [lax.axis_index(n) for n in ("zlo", "zhi", "y")])
    pos = pos.astype(jnp.int32)
    rows, cols, width = tokens.shape
    count = rows * cols

    six = sds((6, 32, 128), BF16)
    keep, send = call(
        pack_kernel,
        (six, six),
        pos,
        jnp.transpose(qkv_weight, (1, 0, 2)),
        out_weight.T,
        up_weight,
        down_weight.T,
    )
    wide = call(
        rows_kernel,
        sds((416, 128), BF16),
        pos,
        keep,
        swapped(send),
        qk_gain.reshape(1, 128),
        hidden_gain.reshape(4, 128),
    )

    pair = jnp.stack([wide, swapped(wide, "zlo")])
    gains = pair[:, 384:]
    quad = direct4(pair[:, :384], "zhi")
    one = jnp.stack([b[:, :192] for b in quad])
    two = jnp.concatenate([b[:, 192:].reshape(384, 128) for b in quad] + [gains.reshape(64, 128)])
    one = direct4(one, "y")
    two = direct4(two, "x")
    gains = jnp.stack([b[1536:].reshape(2, 4, 8, 128) for b in two], 1).astype(F32)
    gains = gains[:, :, 0] + gains[:, :, 1] + gains[:, :, 2]
    head_gain = gains[:, :, 0].reshape(8, 128)
    unit_gain = gains[:, :, 1:3].reshape(8, 256)
    two = [b[:1536].reshape(4, 2, 192, 128) for b in two]
    qk = direct4(jnp.stack([b[:, :, :64] for b in one]), "x")
    vo = direct4(jnp.stack([b[:, :, :64] for b in two]), "y")

    shift_row = shifts[0]
    shift_col = jnp.where(shifts[1] > 8, shifts[1] - WIN, shifts[1])
    nxt_rows = from_offset(tokens[:WIN], ROW, 1)
    rolled = lax.dynamic_slice_in_dim(jnp.concatenate([tokens, nxt_rows], 0), shift_row, rows, 0)
    mine = jnp.stack([rolled, across_edge(rolled)])
    theirs = swapped(mine)
    left, right = jnp.where(first, mine, theirs), jnp.where(first, theirs, mine)
    ext = jnp.concatenate([left[1], left[0], right[0], right[1]], axis=1)
    win = lax.dynamic_slice_in_dim(ext, cols + shift_col, WIN, 1).reshape(2 * count, width)

    mlp_x = jnp.stack([b[:, :, i : i + 64] for i in (64, 128) for b in one])
    mlp_y = jnp.stack([b[:, :, i : i + 64] for i in (64, 128) for b in two])
    mlp_x, mlp_y = (m.reshape(2, 4, *m.shape[1:]) for m in (mlp_x, mlp_y))
    win, mlp_x, mlp_y = lax.optimization_barrier((win, mlp_x, mlp_y))
    mlp_x = ring4(mlp_x, "x")
    mlp_y = ring4(mlp_y, "y")

    part = call(
        attn_kernel,
        sds((2 * count, width), BF16),
        pos,
        win,
        head_gain,
        *qk,
        *vo,
        scratch=[pltpu.VMEM((4, 2 * count, 256), BF16)]
        + [pltpu.VMEM((8, 2 * count, 128), BF16)] * 3
        + [pltpu.VMEM((2 * count, 1024), BF16)],
    )
    full = (part.astype(F32) + swapped(part).astype(F32)).astype(BF16)
    full = full.reshape(rows, WIN, width)

    halo = across_edge(jnp.where(first, full[:, :cols], full[:, cols:]))
    ext = jnp.where(
        first, jnp.concatenate([halo, full], axis=1), jnp.concatenate([full, halo], axis=1)
    )
    strip = lax.dynamic_slice_in_dim(ext, cols - shift_col, cols, 1)
    prev_rows = from_offset(strip[rows - WIN :], ROW, -1)
    attn = lax.dynamic_slice_in_dim(
        jnp.concatenate([prev_rows, strip], 0), WIN - shift_row, rows, 0
    ).reshape(count, width)

    mixed, mx = call(
        mix_kernel,
        (sds((count, width), F32), sds((4, count, 256), BF16)),
        pos,
        tokens.reshape(count, width),
        attn,
        attn_rate.reshape(1, width),
    )
    act = call(
        up_kernel, sds((2 * count, 2048), BF16), pos, mx, swapped(mx), unit_gain, *mlp_x, *mlp_y
    )
    own, other = call(
        down_kernel, (sds((count, width), F32), sds((count, width), BF16)), pos, act, *mlp_x, *mlp_y
    )
    result = call(
        last_kernel,
        sds((count, width), BF16),
        pos,
        own,
        swapped(other),
        mixed,
        mlp_rate.reshape(1, width),
    )
    return result.reshape(rows, cols, width)


def solution(mesh):
    fine = Mesh(mesh.devices.reshape(2, 4, 4, 4, 2), ("zlo", "x", "zhi", "y", "core"))
    return jax.shard_map(
        layer,
        mesh=fine,
        in_specs=(
            P(ROW, COL, None),
            P(),
            P(COL, None, ROW),
            P(ROW, COL),
            P(COL, ROW),
            P(ROW, COL),
            P(ROW),
            P(),
            P(),
            P(ROW),
        ),
        out_specs=P(ROW, COL, None),
        check_vma=False,
    )
```

```python
import jax
import jax.numpy as jnp
from jax import lax
from jax.experimental import pallas as pl
from jax.experimental.pallas import tpu as pltpu
from jax.sharding import Mesh, PartitionSpec as P


HD = 64
WIN = 16
ROW = ("zlo", "x")
COL = ("zhi", "y", "core")
F32 = jnp.float32
BF16 = jnp.bfloat16
NT = (((1,), (1,)), ((), ()))


def from_offset(value, axis, offset):
    n = lax.axis_size(axis)
    return lax.ppermute(value, axis, [((i + offset) % n, i) for i in range(n)])


def swapped(value, axis="core"):
    return lax.ppermute(value, axis, [(0, 1), (1, 0)])


def across_edge(value):
    n = lax.axis_size(COL)
    pairs = [((c - 1 if c % 2 == 0 else c + 1) % n, c) for c in range(n)]
    return lax.ppermute(value, COL, pairs)


def direct4(value, axis):
    return [value] + [from_offset(value, axis, d) for d in (1, 2, 3)]


def ring4(value, axis):
    nxt = from_offset(value, axis, 1)
    prv = from_offset(value, axis, -1)
    return [value, nxt, from_offset(nxt, axis, 1), prv]


def call(kernel, outs, *args, scratch=()):
    specs = [pl.BlockSpec(memory_space=pltpu.SMEM)] + [
        pl.BlockSpec(memory_space=pltpu.VMEM) for _ in args[1:]
    ]
    single = not isinstance(outs, (list, tuple))
    out = pl.pallas_call(
        kernel,
        out_shape=outs,
        in_specs=specs,
        out_specs=jax.tree.map(lambda _: pl.BlockSpec(memory_space=pltpu.VMEM), outs),
        scratch_shapes=list(scratch),
        compiler_params=pltpu.CompilerParams(vmem_limit_bytes=48 * 2**20),
    )(*args)
    return out if single else tuple(out)


def sds(shape, dtype):
    return jax.ShapeDtypeStruct(shape, dtype)


def norm(v):
    return v * lax.rsqrt(jnp.mean(v * v, axis=-1, keepdims=True) + 1e-06)


def to_relative(v, y):
    return pltpu.roll(v, lax.rem(256 - 64 * y, 256), 1)


def to_absolute(v, y):
    return pltpu.roll(v, 64 * y, 1)


def pack_kernel(pos, qkv, out_t, up, down_t, keep, send):
    first = pos[0] == 0

    def put(i, lo, hi):
        keep[i] = jnp.where(first, lo, hi)
        send[i] = jnp.where(first, hi, lo)

    q, k, v, o = qkv[0].astype(F32), qkv[1].astype(F32), qkv[2].astype(F32), out_t[...].astype(F32)

    def pair(i, a, b):
        lo = jnp.concatenate([a[:, :64], b[:, :64]], 1).astype(BF16)
        hi = jnp.concatenate([a[:, 64:], b[:, 64:]], 1).astype(BF16)
        put(i, lo, hi)

    pair(0, q, k)
    put(1, down_t[:, :128], down_t[:, 256:384])
    put(2, up[:, :128], up[:, 256:384])
    pair(3, v, o)
    put(4, down_t[:, 128:256], down_t[:, 384:])
    put(5, up[:, 128:256], up[:, 384:])


def rows_kernel(pos, keep, recv, qk_gain, hidden_gain, wide):
    first = pos[0] == 0
    mine = pl.multiple_of(pos[0] * 32, 32)
    other = pl.multiple_of(32 - pos[0] * 32, 32)
    for i in range(6):
        wide[pl.ds(64 * i + mine, 32)] = keep[i]
        wide[pl.ds(64 * i + other, 32)] = recv[i]
    g = qk_gain[...]
    lane = lax.broadcasted_iota(jnp.int32, g.shape, 1)
    turned = pltpu.roll(g, HD, 1)
    g = jnp.where(first == (lane < HD), g, turned)
    h = hidden_gain[...]
    rest = jnp.concatenate([g, jnp.where(first, h[:2], h[2:]), jnp.zeros((5, 128), F32)], 0)
    parts = []
    for _ in range(3):
        parts.append(rest.astype(BF16).astype(F32))
        rest = rest - parts[-1]
    parts.append(jnp.zeros((8, 128), F32))
    wide[384:] = jnp.concatenate(parts, 0).astype(BF16)


def attn_kernel(pos, win, gain, *refs):
    qk, vo, part, (xs, qs, ks, vs, att) = refs[:4], refs[4:8], refs[8], refs[9:]
    zhi, y = pos[2], pos[3]
    s = norm(win[...].astype(F32))
    for z in range(4):
        slab = to_relative(s[:, 256 * z : 256 * z + 256], y)
        xs[lax.rem(z + 4 - zhi, 4)] = slab.astype(BF16)
    x = jnp.concatenate([xs[i] for i in range(4)], 1)
    group = lax.broadcasted_iota(jnp.int32, (256, 256), 0) // HD
    mean = jnp.where(group == lax.broadcasted_iota(jnp.int32, (256, 256), 1) // HD, 1 / HD, 0.0)
    mean = mean.astype(BF16)
    lane = lax.broadcasted_iota(jnp.int32, (512, 128), 1)
    ones = jnp.ones((256, 128), BF16)
    zero = jnp.zeros((512, 128), F32)
    for dx in range(4):

        def stacked(block):
            return jnp.concatenate(
                [
                    jnp.concatenate([block(z, dy, a) for z in range(4) for dy in range(4)], 0)
                    for a in range(2)
                ],
                1,
            )

        wqk = stacked(lambda z, dy, a: qk[dx][dy, z, a])
        wvo = stacked(lambda z, dy, a: vo[dy][dx, z, a])
        pqk = jnp.dot(x, wqk, preferred_element_type=F32)
        pv = jnp.dot(x, wvo, preferred_element_type=F32)
        square = pqk * pqk
        high = square.astype(BF16)
        low = (square - high.astype(F32)).astype(BF16)
        level = jnp.dot(high, mean, preferred_element_type=F32)
        level = level + jnp.dot(low, mean, preferred_element_type=F32)
        pqk = pqk * lax.rsqrt(level + 1e-06)
        for a in range(2):
            both = pqk[:, 128 * a : 128 * a + 128] * gain[a * 4 + dx][None]
            head = a * 4 + dx
            qs[head] = jnp.where(lane < HD, both * (HD**-0.5), zero).astype(BF16)
            ks[head] = pltpu.roll(both, HD, 1).astype(BF16)
            v = pltpu.roll(pv[:, 128 * a : 128 * a + 128], HD, 1)
            vs[head] = jnp.where(lane < HD, zero, v).astype(BF16)

    def heads(i, carry):
        for head in (2 * i, 2 * i + 1):
            for w in range(2):
                t = slice(256 * w, 256 * w + 256)
                score = lax.dot_general(qs[head, t], ks[head, t], NT, preferred_element_type=F32)
                e = jnp.exp(score).astype(BF16)
                rhs = jnp.concatenate([vs[head, t], ones], 1)
                o = jnp.dot(e, rhs, preferred_element_type=F32)
                at = pl.multiple_of(128 * head, 128)
                att[t, pl.ds(at, 128)] = (o[:, :128] / o[:, 128:]).astype(BF16)
        return carry

    lax.fori_loop(0, 4, heads, 0)

    def project(z, carry):
        rhs = jnp.concatenate(
            [
                jnp.concatenate([vo[dy][dx, z, a] for dy in range(4)], 0)
                for a in range(2)
                for dx in range(4)
            ],
            1,
        )
        r = lax.dot_general(att[...], rhs, NT, preferred_element_type=F32)
        at = pl.multiple_of(lax.rem(z + zhi, 4) * 256, 256)
        part[:, pl.ds(at, 256)] = to_absolute(r, y).astype(BF16)
        return carry

    lax.fori_loop(0, 4, project, 0)


def mix_kernel(pos, tokens, attn, rate, mixed, mx):
    zhi, y = pos[2], pos[3]

    def chunk(i, carry):
        t = pl.ds(pl.multiple_of(128 * i, 128), 128)
        s = norm(tokens[t].astype(F32))
        m = norm(s + rate[...] * (norm(attn[t].astype(F32)) - s))
        mixed[t] = m
        for z in range(4):
            slab = to_relative(m[:, 256 * z : 256 * z + 256], y)
            mx[lax.rem(z + 4 - zhi, 4), t] = slab.astype(BF16)
        return carry

    lax.fori_loop(0, 2, chunk, 0)


def up_kernel(pos, own, other, gain, *refs):
    over_x, over_y, act = refs[:4], refs[4:8], refs[8]
    x = jnp.concatenate(
        [jnp.concatenate([half[z] for z in range(4)], 1) for half in (own, other)], 0
    )
    for a in range(2):
        for dx in range(4):
            blocks = [(z, dy) for z in range(4) for dy in range(4)]
            w = jnp.concatenate(
                [
                    jnp.concatenate(
                        [over_x[dx][1, dy, z, a] for z, dy in blocks], 0
                    ),
                    jnp.concatenate(
                        [over_y[dy][1, dx, z, a] for z, dy in blocks], 0
                    ),
                ],
                1,
            )
            unit = a * 4 + dx
            r = jnp.dot(x, w, preferred_element_type=F32) * gain[unit][None]
            r = 0.5 * r * (1.0 + lax.erf(r * (0.5**0.5)))
            act[:, 256 * unit : 256 * unit + 256] = r.astype(BF16)


def down_kernel(pos, act, *refs):
    over_x, over_y, own, other = refs[:4], refs[4:8], refs[8], refs[9]
    zhi, y = pos[2], pos[3]

    x = act[...]
    for z in range(4):
        rhs = []
        for a in range(2):
            for dx in range(4):
                lo = [over_x[dx][0, dy, z, a] for dy in range(4)]
                hi = [over_y[dy][0, dx, z, a] for dy in range(4)]
                rhs += [jnp.concatenate(lo, 0), jnp.concatenate(hi, 0)]
        r = lax.dot_general(x, jnp.concatenate(rhs, 1), NT, preferred_element_type=F32)
        r = to_absolute(r, y)
        at = pl.multiple_of(lax.rem(z + zhi, 4) * 256, 256)
        own[:, pl.ds(at, 256)] = r[:256]
        other[:, pl.ds(at, 256)] = r[256:].astype(BF16)


def last_kernel(pos, own, recv, mixed, rate, out):
    def chunk(i, carry):
        t = pl.ds(pl.multiple_of(128 * i, 128), 128)
        m = mixed[t]
        mlp = own[t] + recv[t].astype(F32)
        out[t] = norm(m + rate[...] * (norm(mlp) - m)).astype(BF16)
        return carry

    lax.fori_loop(0, 2, chunk, 0)


def layer(
    tokens, shifts, qkv_weight, out_weight, up_weight, down_weight, qk_gain, attn_rate, mlp_rate, hidden_gain
):
    core = lax.axis_index("core")
    first = core == 0
    pos = jnp.stack([core] + [lax.axis_index(n) for n in ("zlo", "zhi", "y")])
    pos = pos.astype(jnp.int32)
    rows, cols, width = tokens.shape
    count = rows * cols

    six = sds((6, 32, 128), BF16)
    keep, send = call(
        pack_kernel,
        (six, six),
        pos,
        jnp.transpose(qkv_weight, (1, 0, 2)),
        out_weight.T,
        up_weight,
        down_weight.T,
    )
    wide = call(
        rows_kernel,
        sds((416, 128), BF16),
        pos,
        keep,
        swapped(send),
        qk_gain.reshape(1, 128),
        hidden_gain.reshape(4, 128),
    )

    pair = jnp.stack([wide, swapped(wide, "zlo")])
    gains = pair[:, 384:]
    quad = direct4(pair[:, :384], "zhi")
    one = jnp.stack([b[:, :192] for b in quad])
    values = [b[:, 192:256].reshape(128, 128) for b in quad] + [gains.reshape(64, 128)]
    values = direct4(jnp.concatenate(values), "x")
    one = direct4(one, "y")
    two = direct4(jnp.stack([b[:, 256:] for b in quad]), "x")
    gains = jnp.stack([b[512:].reshape(2, 4, 8, 128) for b in values], 1).astype(F32)
    gains = gains[:, :, 0] + gains[:, :, 1] + gains[:, :, 2]
    head_gain = gains[:, :, 0].reshape(8, 128)
    unit_gain = gains[:, :, 1:3].reshape(8, 256)
    qk = direct4(jnp.stack([b[:, :, :64] for b in one]), "x")
    vo = direct4(jnp.stack([b[:512].reshape(4, 2, 64, 128) for b in values]), "y")

    shift_row = shifts[0]
    shift_col = jnp.where(shifts[1] > 8, shifts[1] - WIN, shifts[1])
    nxt_rows = from_offset(tokens[:WIN], ROW, 1)
    rolled = lax.dynamic_slice_in_dim(jnp.concatenate([tokens, nxt_rows], 0), shift_row, rows, 0)
    mine = jnp.stack([rolled, across_edge(rolled)])
    theirs = swapped(mine)
    left, right = jnp.where(first, mine, theirs), jnp.where(first, theirs, mine)
    ext = jnp.concatenate([left[1], left[0], right[0], right[1]], axis=1)
    win = lax.dynamic_slice_in_dim(ext, cols + shift_col, WIN, 1).reshape(2 * count, width)

    mlp_x = jnp.stack([b[:, :, i : i + 64] for i in (64, 128) for b in one])
    mlp_y = jnp.stack([b[:, :, i : i + 64] for i in (0, 64) for b in two])
    mlp_x, mlp_y = (m.reshape(2, 4, *m.shape[1:]) for m in (mlp_x, mlp_y))
    win, mlp_x, mlp_y = lax.optimization_barrier((win, mlp_x, mlp_y))
    mlp_x = ring4(mlp_x, "x")
    mlp_y = ring4(mlp_y, "y")

    part = call(
        attn_kernel,
        sds((2 * count, width), BF16),
        pos,
        win,
        head_gain,
        *qk,
        *vo,
        scratch=[pltpu.VMEM((4, 2 * count, 256), BF16)]
        + [pltpu.VMEM((8, 2 * count, 128), BF16)] * 3
        + [pltpu.VMEM((2 * count, 1024), BF16)],
    )
    full = (part.astype(F32) + swapped(part).astype(F32)).astype(BF16)
    full = full.reshape(rows, WIN, width)

    halo = across_edge(jnp.where(first, full[:, :cols], full[:, cols:]))
    ext = jnp.where(
        first, jnp.concatenate([halo, full], axis=1), jnp.concatenate([full, halo], axis=1)
    )
    strip = lax.dynamic_slice_in_dim(ext, cols - shift_col, cols, 1)
    prev_rows = from_offset(strip[rows - WIN :], ROW, -1)
    attn = lax.dynamic_slice_in_dim(
        jnp.concatenate([prev_rows, strip], 0), WIN - shift_row, rows, 0
    ).reshape(count, width)

    mixed, mx = call(
        mix_kernel,
        (sds((count, width), F32), sds((4, count, 256), BF16)),
        pos,
        tokens.reshape(count, width),
        attn,
        attn_rate.reshape(1, width),
    )
    act = call(
        up_kernel, sds((2 * count, 2048), BF16), pos, mx, swapped(mx), unit_gain, *mlp_x, *mlp_y
    )
    own, other = call(
        down_kernel, (sds((count, width), F32), sds((count, width), BF16)), pos, act, *mlp_x, *mlp_y
    )
    result = call(
        last_kernel,
        sds((count, width), BF16),
        pos,
        own,
        swapped(other),
        mixed,
        mlp_rate.reshape(1, width),
    )
    return result.reshape(rows, cols, width)


def solution(mesh):
    fine = Mesh(mesh.devices.reshape(2, 4, 4, 4, 2), ("zlo", "x", "zhi", "y", "core"))
    return jax.shard_map(
        layer,
        mesh=fine,
        in_specs=(
            P(ROW, COL, None),
            P(),
            P(COL, None, ROW),
            P(ROW, COL),
            P(COL, ROW),
            P(ROW, COL),
            P(ROW),
            P(),
            P(),
            P(ROW),
        ),
        out_specs=P(ROW, COL, None),
        check_vma=False,
    )
```

```python
import jax
import jax.numpy as jnp
from jax import lax
from jax.experimental import pallas as pl
from jax.experimental.pallas import tpu as pltpu
from jax.sharding import Mesh, PartitionSpec as P


HD = 64
WIN = 16
ROW = ("zlo", "x")
COL = ("zhi", "y", "core")
F32 = jnp.float32
BF16 = jnp.bfloat16
NT = (((1,), (1,)), ((), ()))


def from_offset(value, axis, offset):
    n = lax.axis_size(axis)
    return lax.ppermute(value, axis, [((i + offset) % n, i) for i in range(n)])


def swapped(value, axis="core"):
    return lax.ppermute(value, axis, [(0, 1), (1, 0)])


def across_edge(value):
    n = lax.axis_size(COL)
    pairs = [((c - 1 if c % 2 == 0 else c + 1) % n, c) for c in range(n)]
    return lax.ppermute(value, COL, pairs)


def direct4(value, axis):
    return [value] + [from_offset(value, axis, d) for d in (1, 2, 3)]


def ring4(value, axis):
    nxt = from_offset(value, axis, 1)
    prv = from_offset(value, axis, -1)
    return [value, nxt, from_offset(nxt, axis, 1), prv]


def call(kernel, outs, *args, scratch=()):
    specs = [pl.BlockSpec(memory_space=pltpu.SMEM)] + [
        pl.BlockSpec(memory_space=pltpu.VMEM) for _ in args[1:]
    ]
    single = not isinstance(outs, (list, tuple))
    out = pl.pallas_call(
        kernel,
        out_shape=outs,
        in_specs=specs,
        out_specs=jax.tree.map(lambda _: pl.BlockSpec(memory_space=pltpu.VMEM), outs),
        scratch_shapes=list(scratch),
        compiler_params=pltpu.CompilerParams(vmem_limit_bytes=48 * 2**20),
    )(*args)
    return out if single else tuple(out)


def sds(shape, dtype):
    return jax.ShapeDtypeStruct(shape, dtype)


def norm(v):
    return v * lax.rsqrt(jnp.mean(v * v, axis=-1, keepdims=True) + 1e-06)


def to_relative(v, y):
    return pltpu.roll(v, lax.rem(256 - 64 * y, 256), 1)


def to_absolute(v, y):
    return pltpu.roll(v, 64 * y, 1)


def pack_kernel(pos, qkv, out_t, up, down_t, keep, send):
    first = pos[0] == 0

    def put(i, lo, hi):
        keep[i] = jnp.where(first, lo, hi)
        send[i] = jnp.where(first, hi, lo)

    q, k, v, o = qkv[0].astype(F32), qkv[1].astype(F32), qkv[2].astype(F32), out_t[...].astype(F32)

    def pair(i, a, b):
        lo = jnp.concatenate([a[:, :64], b[:, :64]], 1).astype(BF16)
        hi = jnp.concatenate([a[:, 64:], b[:, 64:]], 1).astype(BF16)
        put(i, lo, hi)

    pair(0, q, k)
    put(1, down_t[:, :128], down_t[:, 256:384])
    put(2, up[:, :128], up[:, 256:384])
    pair(3, v, o)
    put(4, down_t[:, 128:256], down_t[:, 384:])
    put(5, up[:, 128:256], up[:, 384:])


def rows_kernel(pos, keep, recv, qk_gain, hidden_gain, wide):
    first = pos[0] == 0
    mine = pl.multiple_of(pos[0] * 32, 32)
    other = pl.multiple_of(32 - pos[0] * 32, 32)
    for i in range(6):
        wide[pl.ds(64 * i + mine, 32)] = keep[i]
        wide[pl.ds(64 * i + other, 32)] = recv[i]
    g = qk_gain[...]
    lane = lax.broadcasted_iota(jnp.int32, g.shape, 1)
    turned = pltpu.roll(g, HD, 1)
    g = jnp.where(first == (lane < HD), g, turned)
    h = hidden_gain[...]
    rest = jnp.concatenate([g, jnp.where(first, h[:2], h[2:]), jnp.zeros((5, 128), F32)], 0)
    parts = []
    for _ in range(3):
        parts.append(rest.astype(BF16).astype(F32))
        rest = rest - parts[-1]
    parts.append(jnp.zeros((8, 128), F32))
    wide[384:] = jnp.concatenate(parts, 0).astype(BF16)


def stacked(block):
    return jnp.concatenate(
        [
            jnp.concatenate([block(z, dy, a) for z in range(4) for dy in range(4)], 0)
            for a in range(2)
        ],
        1,
    )


def score_kernel(pos, win, gain, *refs):
    qk, xo, expo, (xs, qs, ks) = refs[:4], refs[4], refs[5], refs[6:]
    zhi, y = pos[2], pos[3]
    s = norm(win[...].astype(F32))
    for z in range(4):
        slab = to_relative(s[:, 256 * z : 256 * z + 256], y)
        xs[lax.rem(z + 4 - zhi, 4)] = slab.astype(BF16)
    x = jnp.concatenate([xs[i] for i in range(4)], 1)
    xo[...] = x
    group = lax.broadcasted_iota(jnp.int32, (256, 256), 0) // HD
    mean = jnp.where(group == lax.broadcasted_iota(jnp.int32, (256, 256), 1) // HD, 1 / HD, 0.0)
    mean = mean.astype(BF16)
    lane = lax.broadcasted_iota(jnp.int32, (512, 128), 1)
    zero = jnp.zeros((512, 128), F32)
    for dx in range(4):
        wqk = stacked(lambda z, dy, a: qk[dx][dy, z, a])
        pqk = jnp.dot(x, wqk, preferred_element_type=F32)
        square = pqk * pqk
        high = square.astype(BF16)
        low = (square - high.astype(F32)).astype(BF16)
        level = jnp.dot(high, mean, preferred_element_type=F32)
        level = level + jnp.dot(low, mean, preferred_element_type=F32)
        pqk = pqk * lax.rsqrt(level + 1e-06)
        for a in range(2):
            both = pqk[:, 128 * a : 128 * a + 128] * gain[a * 4 + dx][None]
            head = a * 4 + dx
            qs[head] = jnp.where(lane < HD, both * (HD**-0.5), zero).astype(BF16)
            ks[head] = pltpu.roll(both, HD, 1).astype(BF16)

    def heads(i, carry):
        for head in (2 * i, 2 * i + 1):
            for w in range(2):
                t = slice(256 * w, 256 * w + 256)
                score = lax.dot_general(qs[head, t], ks[head, t], NT, preferred_element_type=F32)
                expo[head, t] = jnp.exp(score).astype(BF16)
        return carry

    lax.fori_loop(0, 4, heads, 0)


def value_kernel(pos, x, expo, *refs):
    vo, part, (vs, att) = refs[:4], refs[4], refs[5:]
    zhi, y = pos[2], pos[3]
    lane = lax.broadcasted_iota(jnp.int32, (512, 128), 1)
    ones = jnp.ones((256, 128), BF16)
    zero = jnp.zeros((512, 128), F32)
    for dx in range(4):
        wvo = stacked(lambda z, dy, a: vo[dy][dx, z, a])
        pv = jnp.dot(x[...], wvo, preferred_element_type=F32)
        for a in range(2):
            v = pltpu.roll(pv[:, 128 * a : 128 * a + 128], HD, 1)
            vs[a * 4 + dx] = jnp.where(lane < HD, zero, v).astype(BF16)

    def heads(i, carry):
        for head in (2 * i, 2 * i + 1):
            for w in range(2):
                t = slice(256 * w, 256 * w + 256)
                rhs = jnp.concatenate([vs[head, t], ones], 1)
                o = jnp.dot(expo[head, t], rhs, preferred_element_type=F32)
                at = pl.multiple_of(128 * head, 128)
                att[t, pl.ds(at, 128)] = (o[:, :128] / o[:, 128:]).astype(BF16)
        return carry

    lax.fori_loop(0, 4, heads, 0)

    def project(z, carry):
        rhs = jnp.concatenate(
            [
                jnp.concatenate([vo[dy][dx, z, a] for dy in range(4)], 0)
                for a in range(2)
                for dx in range(4)
            ],
            1,
        )
        r = lax.dot_general(att[...], rhs, NT, preferred_element_type=F32)
        at = pl.multiple_of(lax.rem(z + zhi, 4) * 256, 256)
        part[:, pl.ds(at, 256)] = to_absolute(r, y).astype(BF16)
        return carry

    lax.fori_loop(0, 4, project, 0)


def mix_kernel(pos, tokens, attn, rate, mixed, mx):
    zhi, y = pos[2], pos[3]

    def chunk(i, carry):
        t = pl.ds(pl.multiple_of(128 * i, 128), 128)
        s = norm(tokens[t].astype(F32))
        m = norm(s + rate[...] * (norm(attn[t].astype(F32)) - s))
        mixed[t] = m
        for z in range(4):
            slab = to_relative(m[:, 256 * z : 256 * z + 256], y)
            mx[lax.rem(z + 4 - zhi, 4), t] = slab.astype(BF16)
        return carry

    lax.fori_loop(0, 2, chunk, 0)


def up_kernel(pos, own, other, gain, *refs):
    over_x, over_y, act = refs[:4], refs[4:8], refs[8]
    x = jnp.concatenate(
        [jnp.concatenate([half[z] for z in range(4)], 1) for half in (own, other)], 0
    )
    for a in range(2):
        for dx in range(4):
            blocks = [(z, dy) for z in range(4) for dy in range(4)]
            w = jnp.concatenate(
                [
                    jnp.concatenate(
                        [over_x[dx][1, dy, z, a] for z, dy in blocks], 0
                    ),
                    jnp.concatenate(
                        [over_y[dy][1, dx, z, a] for z, dy in blocks], 0
                    ),
                ],
                1,
            )
            unit = a * 4 + dx
            r = jnp.dot(x, w, preferred_element_type=F32) * gain[unit][None]
            r = 0.5 * r * (1.0 + lax.erf(r * (0.5**0.5)))
            act[:, 256 * unit : 256 * unit + 256] = r.astype(BF16)


def down_kernel(pos, act, *refs):
    over_x, over_y, own, other = refs[:4], refs[4:8], refs[8], refs[9]
    zhi, y = pos[2], pos[3]

    x = act[...]
    for z in range(4):
        rhs = []
        for a in range(2):
            for dx in range(4):
                lo = [over_x[dx][0, dy, z, a] for dy in range(4)]
                hi = [over_y[dy][0, dx, z, a] for dy in range(4)]
                rhs += [jnp.concatenate(lo, 0), jnp.concatenate(hi, 0)]
        r = lax.dot_general(x, jnp.concatenate(rhs, 1), NT, preferred_element_type=F32)
        r = to_absolute(r, y)
        at = pl.multiple_of(lax.rem(z + zhi, 4) * 256, 256)
        own[:, pl.ds(at, 256)] = r[:256]
        other[:, pl.ds(at, 256)] = r[256:].astype(BF16)


def last_kernel(pos, own, recv, mixed, rate, out):
    def chunk(i, carry):
        t = pl.ds(pl.multiple_of(128 * i, 128), 128)
        m = mixed[t]
        mlp = own[t] + recv[t].astype(F32)
        out[t] = norm(m + rate[...] * (norm(mlp) - m)).astype(BF16)
        return carry

    lax.fori_loop(0, 2, chunk, 0)


def layer(
    tokens, shifts, qkv_weight, out_weight, up_weight, down_weight, qk_gain, attn_rate, mlp_rate, hidden_gain
):
    core = lax.axis_index("core")
    first = core == 0
    pos = jnp.stack([core] + [lax.axis_index(n) for n in ("zlo", "zhi", "y")])
    pos = pos.astype(jnp.int32)
    rows, cols, width = tokens.shape
    count = rows * cols

    six = sds((6, 32, 128), BF16)
    keep, send = call(
        pack_kernel,
        (six, six),
        pos,
        jnp.transpose(qkv_weight, (1, 0, 2)),
        out_weight.T,
        up_weight,
        down_weight.T,
    )
    wide = call(
        rows_kernel,
        sds((416, 128), BF16),
        pos,
        keep,
        swapped(send),
        qk_gain.reshape(1, 128),
        hidden_gain.reshape(4, 128),
    )

    pair = jnp.stack([wide, swapped(wide, "zlo")])
    gains = pair[:, 384:]
    quad = direct4(pair[:, :384], "zhi")
    one = jnp.stack([b[:, :192] for b in quad])
    two = jnp.concatenate([b[:, 192:].reshape(384, 128) for b in quad] + [gains.reshape(64, 128)])
    one = direct4(one, "y")
    two = direct4(two, "x")
    gains = jnp.stack([b[1536:].reshape(2, 4, 8, 128) for b in two], 1).astype(F32)
    gains = gains[:, :, 0] + gains[:, :, 1] + gains[:, :, 2]
    head_gain = gains[:, :, 0].reshape(8, 128)
    unit_gain = gains[:, :, 1:3].reshape(8, 256)
    two = [b[:1536].reshape(4, 2, 192, 128) for b in two]
    qk = direct4(jnp.stack([b[:, :, :64] for b in one]), "x")
    vo = direct4(jnp.stack([b[:, :, :64] for b in two]), "y")

    shift_row = shifts[0]
    shift_col = jnp.where(shifts[1] > 8, shifts[1] - WIN, shifts[1])
    nxt_rows = from_offset(tokens[:WIN], ROW, 1)
    rolled = lax.dynamic_slice_in_dim(jnp.concatenate([tokens, nxt_rows], 0), shift_row, rows, 0)
    mine = jnp.stack([rolled, across_edge(rolled)])
    theirs = swapped(mine)
    left, right = jnp.where(first, mine, theirs), jnp.where(first, theirs, mine)
    ext = jnp.concatenate([left[1], left[0], right[0], right[1]], axis=1)
    win = lax.dynamic_slice_in_dim(ext, cols + shift_col, WIN, 1).reshape(2 * count, width)

    mlp_x = jnp.stack([b[:, :, i : i + 64] for i in (64, 128) for b in one])
    mlp_y = jnp.stack([b[:, :, i : i + 64] for i in (64, 128) for b in two])
    mlp_x, mlp_y = (m.reshape(2, 4, *m.shape[1:]) for m in (mlp_x, mlp_y))
    win, mlp_x, mlp_y = lax.optimization_barrier((win, mlp_x, mlp_y))
    mlp_x = ring4(mlp_x, "x")
    mlp_y = ring4(mlp_y, "y")

    x, expo = call(
        score_kernel,
        (sds((2 * count, width), BF16), sds((8, 2 * count, 256), BF16)),
        pos,
        win,
        head_gain,
        *qk,
        scratch=[pltpu.VMEM((4, 2 * count, 256), BF16)]
        + [pltpu.VMEM((8, 2 * count, 128), BF16)] * 2,
    )
    part = call(
        value_kernel,
        sds((2 * count, width), BF16),
        pos,
        x,
        expo,
        *vo,
        scratch=[pltpu.VMEM((8, 2 * count, 128), BF16), pltpu.VMEM((2 * count, 1024), BF16)],
    )
    full = (part.astype(F32) + swapped(part).astype(F32)).astype(BF16)
    full = full.reshape(rows, WIN, width)

    halo = across_edge(jnp.where(first, full[:, :cols], full[:, cols:]))
    ext = jnp.where(
        first, jnp.concatenate([halo, full], axis=1), jnp.concatenate([full, halo], axis=1)
    )
    strip = lax.dynamic_slice_in_dim(ext, cols - shift_col, cols, 1)
    prev_rows = from_offset(strip[rows - WIN :], ROW, -1)
    attn = lax.dynamic_slice_in_dim(
        jnp.concatenate([prev_rows, strip], 0), WIN - shift_row, rows, 0
    ).reshape(count, width)

    mixed, mx = call(
        mix_kernel,
        (sds((count, width), F32), sds((4, count, 256), BF16)),
        pos,
        tokens.reshape(count, width),
        attn,
        attn_rate.reshape(1, width),
    )
    act = call(
        up_kernel, sds((2 * count, 2048), BF16), pos, mx, swapped(mx), unit_gain, *mlp_x, *mlp_y
    )
    own, other = call(
        down_kernel, (sds((count, width), F32), sds((count, width), BF16)), pos, act, *mlp_x, *mlp_y
    )
    result = call(
        last_kernel,
        sds((count, width), BF16),
        pos,
        own,
        swapped(other),
        mixed,
        mlp_rate.reshape(1, width),
    )
    return result.reshape(rows, cols, width)


def solution(mesh):
    fine = Mesh(mesh.devices.reshape(2, 4, 4, 4, 2), ("zlo", "x", "zhi", "y", "core"))
    return jax.shard_map(
        layer,
        mesh=fine,
        in_specs=(
            P(ROW, COL, None),
            P(),
            P(COL, None, ROW),
            P(ROW, COL),
            P(COL, ROW),
            P(ROW, COL),
            P(ROW),
            P(),
            P(),
            P(ROW),
        ),
        out_specs=P(ROW, COL, None),
        check_vma=False,
    )
```
